512 devices in a mesh: dimer: 128 (over x, z, core), rep: 4 (over y).
Axes of the slice: x: 4, y: 4, z: 16, core: 2. Of those that a mesh axis runs over, the one named last changes fastest.
Arguments:
- integrals: bfloat16 [4096, 256, 3, 128], P('dimer', 'rep'), may hold values from -0.375 to 0.375
- density: bfloat16 [4096, 256], P('dimer', 'rep'), may hold values from -6 to 6
- energy_terms: bfloat16 [4096, 256], P('dimer', 'rep'), may hold values from -0.005859375 to 0.005859375
- positions: float32 [3, 262144], P(None, ('dimer', 'rep')), may hold values from -0.01171875 to 0.01171875
- dimer_owners: int32 [4096, 2], P('dimer'), may hold values from 0 to 127, all different within a row; in each aligned block of 32 rows (0 to 31, 32 to 63, ...) at most 2 rows name the same one
- dimer_local: int32 [4096, 2], P('dimer'), may hold values from 0 to 31
Outputs:
- forces: float32 [3, 262144], P(None, ('dimer', 'rep'))
- energy: float32 [], replicated
- virial: float32 [], replicated
The draws below stay inside these ranges and needn't reach their ends.
Inputs may be any that keep to these rules, and one draw needn't show every extreme that they name: `dimer_owners`: the two entries of a row differ. Among the 32 rows of one device no value stands more than 2 times, and some value stands exactly 2 times in some device's rows.
All inputs are finite; a program needn't handle non-finite values.
Results may differ from the reference program's by a relative error of at most 0.00045.
Values sent between devices are 32-bit elements; how exact they have to be, the bound alone decides.
No kernel may reach another device: no remote copies, remote signals or barrier semaphores. Data moves between devices by JAX's collectives and lax.ppermute only.
A program may use at most 64 MiB of HBM per device.

```python
import math
import jax
import jax.numpy as jnp
import numpy as np
from jax import lax

A = 64
NTERMS = 256
FRAG_DEV = 32
DIM_DEV = 32
OWNERS = 128
FRAGMENTS = 4096
ATOMS = 262144
DIMERS = 4096
CAP = 2


def plant(result, stream_key, least, largest):
    extent = result.shape
    place = [jax.random.randint(jax.random.fold_in(stream_key, axis), (), 0, extent[axis]) for axis in range(len(extent))]
    result = result.at[tuple(place)].set(least)
    longest = extent.index(max(extent))
    place[longest] = (place[longest] + 1) % extent[longest]
    return result.at[tuple(place)].set(largest)


def steps_of(own_key, dims, shards, smallest, high):
    factor_of, own = 1.0, jax.random.fold_in(own_key, 6)
    for position, blocks in shards:
        draws = jnp.exp(jax.random.uniform(jax.random.fold_in(own, position), (blocks,), jnp.float32, smallest / len(shards), high / len(shards)))
        factor_of = factor_of * jnp.repeat(draws, dims[position] // blocks).reshape([-1 if axis == position else 1 for axis in range(len(dims))])
    return factor_of


def deal_out(stream_key, own, number, rows, amount, top, most, lean):
    order = jax.random.permutation(stream_key, amount)
    packed, usual = portions_of(amount, rows * top, most, lean, True), portions_of(amount, rows * top, most, lean, False)
    places = jnp.arange(amount)

    def named(tallies, rotation):
        used = int((tallies > 0).sum())
        fixed = max(1, used // 4)
        passed = fixed + (places - fixed + rotation * (used - fixed)) % max(1, amount - fixed)
        return jnp.zeros((amount,), jnp.int32).at[order[jnp.where(places < fixed, places, passed)]].set(jnp.asarray(tallies, jnp.int32))

    tallies = jnp.where(number % 4 == 0, named(packed, number // 4), named(usual, number - number // 4 - 1))
    mixed = jax.random.permutation(jax.random.fold_in(own, 3), amount)
    donor, taker = mixed[0:amount // 2 * 2:2], mixed[1:amount // 2 * 2:2]
    slack = jnp.minimum(tallies[donor] - 1, most - tallies[taker]) // 2
    slack = jnp.where((donor == order[0]) | (taker == order[0]) | (tallies[taker] == 0), 0, jnp.maximum(slack, 0))
    passed = jax.random.randint(jax.random.fold_in(own, 4), (amount // 2,), 0, 1 << 20) % (slack + 1)
    tallies = tallies.at[donor].add(-passed).at[taker].add(passed)
    labels = jnp.searchsorted(jnp.cumsum(tallies), jnp.arange(rows * top), side="right").astype(jnp.int32)
    grid = labels.reshape(top, rows).T
    grid = grid[jax.random.permutation(jax.random.fold_in(own, 1), rows)]
    rotation = jax.random.randint(jax.random.fold_in(own, 2), (rows, 1), 0, top)
    return jnp.take_along_axis(grid, (jnp.arange(top)[None, :] + rotation) % top, axis=1)


def portions_of(amount, total, most, slope, full):
    weights = [(1 << 20) // math.isqrt(rank ** slope) + 1 for rank in range(1, amount + 1)]
    largest = most if full else min(most, max(-(-total // amount), total * weights[0] // sum(weights)))
    least = 1 if total - largest >= amount - 1 else 0
    given, surplus = [largest] + [least] * (amount - 1), total - largest - least * (amount - 1)
    while surplus > 0:
        free = [i for i in range(1, amount) if given[i] < largest] or [i for i in range(1, amount) if given[i] < most]
        pool, budget = sum([weights[i] for i in free]), surplus
        for i in free:
            extra = min(most - given[i], max(1, budget * weights[i] // pool), surplus)
            given[i] = given[i] + extra
            surplus = surplus - extra
    return np.array(given)


def normal_values(stream_key, shape, scale, most, cuts=(), kind=jnp.bfloat16):
    values = scale * jax.random.normal(stream_key, shape, jnp.float32)
    if cuts:
        values = values * steps_of(stream_key, shape, cuts, -0.22, 0.18)
    return jnp.clip(values, -most, most).astype(kind)


def setup_inputs(seed: int = 0) -> dict:
    key_of = jax.random.split(jax.random.key(seed), 7)
    integrals = normal_values(key_of[0], (DIMERS, NTERMS, 3, 2 * A), NTERMS ** -0.5, 0.375, ((0, 128), (1, 4)))
    density = normal_values(key_of[1], (DIMERS, NTERMS), 1.0, 6.0, ((0, 128), (1, 4)))
    energy_terms = normal_values(key_of[2], (DIMERS, NTERMS), (NTERMS * DIMERS) ** -0.5, 0.005859375, ((0, 128), (1, 4)))
    positions = normal_values(key_of[3], (3, ATOMS), (ATOMS ** -0.5), 0.01171875, ((1, 512),), jnp.float32)
    dimer_owners_keys = jax.random.split(jax.random.fold_in(key_of[4], 1), DIMERS // DIM_DEV)
    dimer_owners_turns = jax.random.permutation(jax.random.fold_in(key_of[4], 3), DIMERS // DIM_DEV)
    dimer_owners = jax.vmap(lambda own, number: deal_out(jax.random.fold_in(key_of[4], 2), own, number, DIM_DEV, OWNERS, 2, CAP, 2))(dimer_owners_keys, dimer_owners_turns).reshape((DIMERS, 2))
    dimer_local = plant(jax.random.randint(key_of[5], (DIMERS, 2), 0, FRAG_DEV), jax.random.fold_in(key_of[5], 1), 0, FRAG_DEV - 1).astype(jnp.int32)
    return dict(integrals=integrals, density=density, energy_terms=energy_terms, positions=positions, dimer_owners=dimer_owners, dimer_local=dimer_local)


def contract(block):
    weights, ints = block
    return jnp.einsum("sk,skcb->scb", weights.astype(jnp.float32), ints.astype(jnp.float32))


def reference(integrals, density, energy_terms, positions, dimer_owners, dimer_local):
    grads = lax.map(contract, (density.reshape(OWNERS, DIM_DEV, NTERMS), integrals.reshape(OWNERS, DIM_DEV, NTERMS, 3, 2 * A)))
    grads = grads.reshape(DIMERS, 3, 2, A)
    pieces = jnp.transpose(grads, (0, 2, 1, 3)).reshape(DIMERS * 2, 3, A)
    fragment = (dimer_owners * FRAG_DEV + dimer_local).reshape(-1).astype(jnp.int32)
    summed = jax.ops.segment_sum(pieces, fragment, num_segments=FRAGMENTS)
    forces = jnp.transpose(summed, (1, 0, 2)).reshape(3, ATOMS)
    energy = jnp.sum(density.astype(jnp.float32) * energy_terms.astype(jnp.float32))
    virial = -jnp.sum(positions * forces) / 3.0
    return forces, energy, virial
```

```python
import jax
import jax.numpy as jnp
from jax import lax
from jax.experimental import pallas as pl
from jax.experimental.pallas import tpu as pltpu
from jax.sharding import Mesh
from jax.sharding import PartitionSpec as P

X, Z, C, Y = 4, 16, 2, 4
XC = X * C
PLANE = XC * Y
AT = 64
SLOTS = 32
LOC, NRG = 192, 193
DIMER = ("x", "z", "c")
ALL = ("x", "z", "c", "y")
f32, bf16, i32 = jnp.float32, jnp.bfloat16, jnp.int32


def iota(shape, dim):
    return lax.broadcasted_iota(i32, shape, dim)


def split(v):
    hi = v.astype(bf16)
    return hi, (v - hi.astype(f32)).astype(bf16)


def dot(a, b, dims=((1,), (0,))):
    return lax.dot_general(a, b, (dims, ((), ())), preferred_element_type=f32)


def swap(v):
    return pltpu.roll(v, AT, 1)


def pair(a, b):
    return jnp.where(iota(a.shape, 1) < AT, a, b)


def send_kernel(h_ints, h_dens, h_terms, h_own, h_loc, h_pos, out, pos_out, *scratch):
    ints, dens, terms, own, loc, pos, sems = scratch
    sources = (h_own, h_loc, h_pos, h_dens, h_terms, h_ints)
    copies = [
        pltpu.make_async_copy(a, b, sems.at[i])
        for i, (a, b) in enumerate(zip(sources, (own, loc, pos, dens, terms, ints)))
    ]
    for copy in copies:
        copy.start()
    for copy in copies:
        copy.wait()

    d = dens[...].astype(f32)
    dd = jnp.concatenate([d, d], axis=1)
    row, half = iota(dd.shape, 0), iota(dd.shape, 1) // AT
    diag = jnp.concatenate(
        [jnp.where(row == 2 * j + half, dd, 0.0).astype(bf16) for j in range(SLOTS // 2)], axis=1
    )
    g0, g1, g2 = (dot(diag, ints[:, c].reshape(SLOTS * AT, 2 * AT)) for c in range(3))
    energy = jnp.sum(d * terms[...].astype(f32))

    o = jnp.concatenate([own[0:1], own[1:2]] * 2, axis=1)
    z, xc = (o >> 1) & (Z - 1), (o >> 5) * C + (o & 1)
    e = (iota((Z * XC, 4 * SLOTS), 0) == z * XC + xc).astype(bf16)
    p, q = iota((4 * SLOTS, 4 * SLOTS), 0), iota((4 * SLOTS, 4 * SLOTS), 1)
    before = ((p < 2 * SLOTS) & (p < q % (2 * SLOTS))).astype(bf16)
    count = dot(e, before)
    e3, count3 = e.astype(f32).reshape(Z, 1, XC, 4 * SLOTS), count.reshape(Z, 1, XC, 4 * SLOTS)
    route = jnp.concatenate([jnp.where(count3 == r, e3, 0.0) for r in (0.0, 1.0)], axis=1)
    route = route.reshape(Z * 2 * XC, 4 * SLOTS).astype(bf16)

    same = iota((SLOTS, SLOTS), 0) == iota((SLOTS, SLOTS), 1)
    places = [
        jnp.sum(jnp.where(same, loc[t : t + 1].astype(f32), 0.0), axis=1, keepdims=True)
        for t in range(2)
    ]
    places = [jnp.broadcast_to(v, (SLOTS, 2 * AT)) for v in places]
    rows = jnp.concatenate(
        [
            jnp.concatenate([pair(g0, swap(g1)), pair(g2, places[0])], axis=1),
            jnp.concatenate([pair(swap(g0), g1), pair(swap(g2), places[1])], axis=1),
        ],
        axis=0,
    )
    sent = dot(route, jnp.concatenate(split(rows), axis=0))
    sent = jnp.where(iota(sent.shape, 1) == NRG, energy, sent)
    out[...] = sent.reshape(Z, 2 * XC, 4 * AT)

    lines = []
    for f in range(8):
        w = pos[:, 2 * AT * (f // 2) : 2 * AT * (f // 2 + 1)]
        s = swap(w)
        a, b = (w, s) if f % 2 == 0 else (s, w)
        zero = jnp.zeros((1, 2 * AT), f32)
        lines.append(
            jnp.concatenate([pair(a[0:1], b[1:2]), pair(a[2:3], zero)], axis=1)
        )
    block = jnp.concatenate(lines, axis=0)
    pos_out[...] = jnp.broadcast_to(block[None], pos_out.shape)


def lane_kernel(got, pos, out):
    v = got[...].reshape(Z * 2 * XC, 4 * AT)
    n = (Z * 2 * XC, PLANE * 8)
    place = v[:, LOC : LOC + 1].astype(i32)
    q = iota(n, 1)
    pick = ((q >> 5) == (iota(n, 0) & (XC - 1))) & ((q & 31) == place)
    pick = pick.astype(f32).astype(bf16)
    hi, lo = split(v)
    lane = dot(pick, hi, ((0,), (0,))) + dot(pick, lo, ((0,), (0,)))
    at = iota(lane.shape, 1)
    virial = -jnp.sum(jnp.where(at < LOC, lane * pos[...].reshape(lane.shape), 0.0)) / 3.0
    first = (iota(v.shape, 0) & (2 * XC - 1)) == 0
    energy = jnp.sum(jnp.where(first & (iota(v.shape, 1) == NRG), v, 0.0)) / Z
    lane = jnp.where(at == LOC, virial, jnp.where(at == NRG, energy, lane))
    out[...] = lane.reshape(PLANE, 8, 4 * AT)


def force_kernel(got, forces, scalars):
    s = jnp.sum(got[...], axis=0)
    u, w = s[:, : 2 * AT], s[:, 2 * AT :]
    su, sw = swap(u), swap(w)
    for k in range(4):
        a, b = slice(2 * k, 2 * k + 1), slice(2 * k + 1, 2 * k + 2)
        cols = slice(2 * AT * k, 2 * AT * (k + 1))
        forces[0:1, cols] = pair(u[a], su[b])
        forces[1:2, cols] = pair(su[a], u[b])
        forces[2:3, cols] = pair(w[a], sw[b])
    scalars[...] = jnp.broadcast_to(w[0:1][None], scalars.shape)


VM = pl.BlockSpec(memory_space=pltpu.VMEM)
HBM = pl.BlockSpec(memory_space=pltpu.HBM)


def call(kernel, outs, n, flops, scratch=(), where=VM):
    return pl.pallas_call(
        kernel,
        out_shape=outs,
        in_specs=[where] * n,
        scratch_shapes=scratch,
        out_specs=jax.tree.map(lambda _: VM, outs),
        cost_estimate=pl.CostEstimate(flops=flops, bytes_accessed=1 << 20, transcendentals=0),
        compiler_params=pltpu.CompilerParams(vmem_limit_bytes=16 << 20),
    )


def arr(*shape):
    return jax.ShapeDtypeStruct(shape, f32)


def on_device(integrals, density, energy_terms, positions, dimer_owners, dimer_local):
    args = (
        jnp.transpose(integrals, (0, 2, 1, 3)),
        density,
        energy_terms,
        dimer_owners.T,
        dimer_local.T,
        positions,
    )
    scratch = [pltpu.VMEM(a.shape, a.dtype) for a in args] + [pltpu.SemaphoreType.DMA((6,))]
    outs = (arr(Z, 2 * XC, 4 * AT), arr(PLANE, 8, 4 * AT))
    sent, pos = call(send_kernel, outs, 6, 4_000_000, scratch, HBM)(
        *(pltpu.with_memory_space_constraint(a, pltpu.HBM) for a in args)
    )
    got = lax.all_to_all(sent, "z", 0, 0, tiled=True)
    pos = lax.all_to_all(pos, ("x", "c", "y"), 0, 0, tiled=True)
    lane = call(lane_kernel, arr(PLANE, 8, 4 * AT), 2, 4_000_000)(got, pos)
    parts = lax.all_to_all(lane, ("x", "c", "y"), 0, 0, tiled=True)
    forces, scalars = call(force_kernel, (arr(3, 8 * AT), arr(Z, 1, 2 * AT)), 1, 1_000_000)(parts)
    totals = jnp.sum(lax.all_to_all(scalars, "z", 0, 0, tiled=True), axis=(0, 1))
    return forces, totals[NRG - 2 * AT], totals[LOC - 2 * AT]


def solution(mesh):
    split_mesh = Mesh(mesh.devices.reshape(X, Z, C, Y), ALL)
    placed = (
        P(DIMER, "y", None, None),
        P(DIMER, "y"),
        P(DIMER, "y"),
        P(None, ALL),
        P(DIMER, None),
        P(DIMER, None),
    )
    return jax.shard_map(
        on_device,
        mesh=split_mesh,
        in_specs=placed,
        out_specs=(P(None, ALL), P(), P()),
        check_vma=False,
    )
```

```python
import jax
import jax.numpy as jnp
from jax import lax
from jax.experimental import pallas as pl
from jax.experimental.pallas import tpu as pltpu
from jax.sharding import Mesh
from jax.sharding import PartitionSpec as P

X, Z, C, Y = 4, 16, 2, 4
XC = X * C
PLANE = XC * Y
AT = 64
W = 128
SLOTS = 32
Q = 48
PLACE, POS, SCALAR = 2 * Q, 98, 127
DIMER = ("x", "z", "c")
ALL = ("x", "z", "c", "y")
f32, bf16, i32 = jnp.float32, jnp.bfloat16, jnp.int32


def iota(shape, dim):
    return lax.broadcasted_iota(i32, shape, dim)


def split(v):
    hi = v.astype(bf16)
    return hi, (v - hi.astype(f32)).astype(bf16)


def dot(a, b, dims=((1,), (0,))):
    return lax.dot_general(a, b, (dims, ((), ())), preferred_element_type=f32)


def turn(v, by):
    by %= W
    return pltpu.roll(v, by, 1) if by else v


def pair(a, b):
    return jnp.where(iota(a.shape, 1) < AT, a, b)


def window(v0, v1, first, count, to):
    lane = iota(v0.shape, 1)
    inside = (lane >= to) & (lane < to + count)
    if first + count <= W:
        v = turn(v0, to - first)
    elif first >= W:
        v = turn(v1, to - first)
    else:
        v = jnp.where(lane < to + W - first, turn(v0, to - first), turn(v1, to - first))
    return jnp.where(inside, v, 0.0)


def send_kernel(h_ints, h_dens, h_terms, h_own, h_loc, h_pos, out, *scratch):
    ints, dens, terms, own, loc, pos, sems = scratch
    sources = (h_own, h_loc, h_pos, h_dens, h_terms, h_ints)
    copies = [
        pltpu.make_async_copy(a, b, sems.at[i])
        for i, (a, b) in enumerate(zip(sources, (own, loc, pos, dens, terms, ints)))
    ]
    for copy in copies:
        copy.start()
    for copy in copies[:-1]:
        copy.wait()

    o = jnp.concatenate([own[0:1], own[1:2]] * 2, axis=1)
    z, xc = (o >> 1) & (Z - 1), (o >> 5) * C + (o & 1)
    e = (iota((XC * Z, W), 0) == xc * Z + z).astype(f32).astype(bf16)
    p, q = iota((W, W), 0), iota((W, W), 1)
    before = ((p < 2 * SLOTS) & (p < q % (2 * SLOTS))).astype(f32).astype(bf16)
    count = dot(e, before)
    rank = (iota((XC * Z, W), 1) >= 2 * SLOTS).astype(f32)
    route = jnp.where(count == rank, e.astype(f32), 0.0).astype(bf16)
    same = iota((SLOTS, SLOTS), 0) == iota((SLOTS, SLOTS), 1)
    places = [
        jnp.sum(jnp.where(same, loc[t : t + 1].astype(f32), 0.0), axis=1, keepdims=True)
        for t in range(2)
    ]
    place = jnp.concatenate([jnp.broadcast_to(v, (SLOTS, W)) for v in places], axis=0)

    lines = []
    for f in range(8):
        w = pos[:, W * (f // 2) : W * (f // 2 + 1)]
        s = turn(w, AT)
        a, b = (w, s) if f % 2 == 0 else (s, w)
        lines.append((pair(a[0:1], b[1:2]), a[2:3]))
    x0, x1 = (jnp.concatenate([line[i] for line in lines], axis=0) for i in range(2))

    d = dens[...].astype(f32)
    energy = jnp.sum(d * terms[...].astype(f32))
    dd = jnp.concatenate([d, d], axis=1)
    row, half = iota(dd.shape, 0), iota(dd.shape, 1) // AT
    diag = jnp.concatenate(
        [jnp.where(row == 2 * j + half, dd, 0.0).astype(bf16) for j in range(SLOTS // 2)], axis=1
    )

    copies[-1].wait()
    g0, g1, g2 = (dot(diag, ints[:, c].reshape(SLOTS * AT, 2 * AT)) for c in range(3))
    v0 = jnp.concatenate([pair(g0, turn(g1, AT)), pair(turn(g0, AT), g1)], axis=0)
    v1 = jnp.concatenate([g2, turn(g2, AT)], axis=0)

    lane = iota((2 * SLOTS, W), 1)
    shares = []
    for y in range(Y):
        rows = [
            jnp.where(lane == PLACE + r, place, window(v0, v1, Q * y, Q, Q * r)) for r in range(2)
        ]
        shares.append(jnp.concatenate(rows, axis=0))
    hi, lo = split(jnp.concatenate(shares, axis=1))
    sent = dot(route, hi) + dot(route, lo)
    at = iota((2 * 8, W), 1)
    for y in range(Y):
        extra = jnp.concatenate(
            [window(x0, x1, Q * y + Q // 2 * h, Q // 2, POS) for h in range(2)], axis=0
        )
        extra = jnp.where(at == SCALAR, energy, extra)
        share = sent[:, W * y : W * (y + 1)].reshape(XC, Z, W)
        for k in range(XC):
            out[k * Y + y] = jnp.where(at < POS, share[k], extra)


def me():
    return lax.axis_index("x") * C + lax.axis_index("c")


def turn_kernel(got, out, pos):
    for k in range(XC):
        s = (got[k * Y] + got[k * Y + 1]) + (got[k * Y + 2] + got[k * Y + 3])
        out[:, k, :] = s
    mine = got[pl.ds(me() * Y, Y)]
    a, b = mine[:, :8].reshape(SLOTS, W), mine[:, 8:].reshape(SLOTS, W)
    a, b = turn(a, -POS), turn(b, Q // 2 - POS)
    lane = iota(a.shape, 1)
    pos[...] = jnp.where(lane < Q // 2, a, jnp.where(lane < Q, b, 0.0))


def block_kernel(got, pos, out):
    v = got[...].reshape(Z * XC, W)
    lane = iota(v.shape, 1)
    f = iota((Z * XC, SLOTS), 1).astype(f32) * Y
    picks, datas = [], []
    for r in range(2):
        picks.append((v[:, PLACE + r : PLACE + r + 1] == f).astype(f32).astype(bf16))
        datas.append(jnp.where(lane < Q, turn(v, -Q * r), 0.0))
    pick = jnp.concatenate(picks, axis=0)
    hi, lo = split(jnp.concatenate(datas, axis=0))
    block = dot(pick, hi, ((0,), (0,))) + dot(pick, lo, ((0,), (0,)))
    virial = -jnp.sum(block * pos[...]) / 3.0
    energy = jnp.sum(jnp.where(lane == SCALAR, v, 0.0)) / (Z * PLANE)
    at = iota(block.shape, 1)
    block = jnp.where(at == SCALAR, energy, jnp.where(at == SCALAR - 1, virial, block))
    for k in range(XC):
        out[k * Y : (k + 1) * Y] = block.reshape(Y, 8, W)


def force_kernel(got, forces, scalars):
    total = jnp.sum(got[:, 0:1, :], axis=0)
    scalars[...] = jnp.broadcast_to(total[None], scalars.shape)
    mine = got[pl.ds(me() * Y, Y)]
    lane = iota((8, W), 1)
    m1, m2 = turn(mine[1], Q), turn(mine[2], 2 * Q)
    u = jnp.where(lane < Q, mine[0], jnp.where(lane < 2 * Q, m1, m2))
    w = jnp.where(lane < 3 * Q - W, m2, turn(mine[3], 3 * Q - W))
    su, sw = turn(u, AT), turn(w, AT)
    for k in range(4):
        a, b = slice(2 * k, 2 * k + 1), slice(2 * k + 1, 2 * k + 2)
        cols = slice(W * k, W * (k + 1))
        forces[0:1, cols] = pair(u[a], su[b])
        forces[1:2, cols] = pair(su[a], u[b])
        forces[2:3, cols] = pair(w[a], sw[b])


VM = pl.BlockSpec(memory_space=pltpu.VMEM)
HBM = pl.BlockSpec(memory_space=pltpu.HBM)


def call(kernel, outs, n, scratch=(), where=VM):
    return pl.pallas_call(
        kernel,
        out_shape=outs,
        in_specs=[where] * n,
        out_specs=jax.tree.map(lambda _: VM, outs),
        scratch_shapes=scratch,
        compiler_params=pltpu.CompilerParams(vmem_limit_bytes=16 << 20),
    )


def arr(*shape):
    return jax.ShapeDtypeStruct(shape, f32)


def exchange(v, axes):
    return lax.all_to_all(v, axes, 0, 0, tiled=True)


def on_device(integrals, density, energy_terms, positions, dimer_owners, dimer_local):
    args = (
        jnp.transpose(integrals, (0, 2, 1, 3)),
        density,
        energy_terms,
        dimer_owners.T,
        dimer_local.T,
        positions,
    )
    scratch = [pltpu.VMEM(a.shape, a.dtype) for a in args] + [pltpu.SemaphoreType.DMA((6,))]
    args = (pltpu.with_memory_space_constraint(a, pltpu.HBM) for a in args)
    v = call(send_kernel, arr(PLANE, Z, W), 6, scratch, HBM)(*args)
    v = exchange(v, ("x", "c", "y"))
    v, pos = call(turn_kernel, (arr(Z, XC, W), arr(SLOTS, W)), 1)(v)
    v = exchange(v, "z")
    v = call(block_kernel, arr(PLANE, 8, W), 2)(v, pos)
    v = exchange(v, ("x", "c", "y"))
    forces, v = call(force_kernel, (arr(3, 8 * AT), arr(Z, 1, W)), 1)(v)
    totals = jnp.sum(exchange(v, "z"), axis=(0, 1))
    return forces, totals[SCALAR], totals[SCALAR - 1]


def solution(mesh):
    split_mesh = Mesh(mesh.devices.reshape(X, Z, C, Y), ALL)
    placed = (
        P(DIMER, "y", None, None),
        P(DIMER, "y"),
        P(DIMER, "y"),
        P(None, ALL),
        P(DIMER, None),
        P(DIMER, None),
    )
    return jax.shard_map(
        on_device,
        mesh=split_mesh,
        in_specs=placed,
        out_specs=(P(None, ALL), P(), P()),
        check_vma=False,
    )
```

```python
import jax
import jax.numpy as jnp
from jax import lax
from jax.experimental import pallas as pl
from jax.experimental.pallas import tpu as pltpu
from jax.sharding import Mesh
from jax.sharding import PartitionSpec as P

X, Z, C, Y = 4, 16, 2, 4
XC = X * C
PLANE = XC * Y
AT = 64
W = 128
SLOTS = 32
Q = 48
PLACE, POS, SCALAR = 2 * Q, 98, 127
X0, C0, Y0, Z0 = 2, 1, 2, 8
ZS = [(Z0 + k) % Z for k in range(Z)]
YS = [(Y0 + k) % Y for k in range(Y)]
XCS = [(X0 + i) % X * C + (C0 + j) % C for i in range(X) for j in range(C)]
DIMER = ("x", "z", "c")
ALL = ("x", "z", "c", "y")
f32, bf16, i32 = jnp.float32, jnp.bfloat16, jnp.int32


def iota(shape, dim):
    return lax.broadcasted_iota(i32, shape, dim)


def split(v):
    hi = v.astype(bf16)
    return hi, (v - hi.astype(f32)).astype(bf16)


def dot(a, b, dims=((1,), (0,))):
    return lax.dot_general(a, b, (dims, ((), ())), preferred_element_type=f32)


def turn(v, by):
    by %= W
    return pltpu.roll(v, by, 1) if by else v


def pair(a, b):
    return jnp.where(iota(a.shape, 1) < AT, a, b)


def window(v0, v1, first, count, to):
    lane = iota(v0.shape, 1)
    inside = (lane >= to) & (lane < to + count)
    if first + count <= W:
        v = turn(v0, to - first)
    elif first >= W:
        v = turn(v1, to - first)
    else:
        v = jnp.where(lane < to + W - first, turn(v0, to - first), turn(v1, to - first))
    return jnp.where(inside, v, 0.0)


def send_kernel(h_ints, h_dens, h_terms, h_own, h_loc, h_pos, out, *scratch):
    ints, dens, terms, own, loc, pos, sems = scratch
    sources = (h_own, h_loc, h_pos, h_dens, h_terms, h_ints)
    copies = [
        pltpu.make_async_copy(a, b, sems.at[i])
        for i, (a, b) in enumerate(zip(sources, (own, loc, pos, dens, terms, ints)))
    ]
    for copy in copies:
        copy.start()
    for copy in copies[:-1]:
        copy.wait()

    o = jnp.concatenate([own[0:1], own[1:2]] * 2, axis=1)
    z = ((o >> 1) - Z0) & (Z - 1)
    xc = (((o >> 5) - X0) & (X - 1)) * C + ((o & 1) ^ C0)
    e = (iota((XC * Z, W), 0) == xc * Z + z).astype(f32).astype(bf16)
    p, q = iota((W, W), 0), iota((W, W), 1)
    before = ((p < 2 * SLOTS) & (p < q % (2 * SLOTS))).astype(f32).astype(bf16)
    count = dot(e, before)
    rank = (iota((XC * Z, W), 1) >= 2 * SLOTS).astype(f32)
    route = jnp.where(count == rank, e.astype(f32), 0.0).astype(bf16)
    same = iota((SLOTS, SLOTS), 0) == iota((SLOTS, SLOTS), 1)
    places = [
        jnp.sum(jnp.where(same, loc[t : t + 1].astype(f32), 0.0), axis=1, keepdims=True)
        for t in range(2)
    ]
    place = jnp.concatenate([jnp.broadcast_to(v, (SLOTS, W)) for v in places], axis=0)

    lines = []
    for f in range(8):
        w = pos[:, W * (f // 2) : W * (f // 2 + 1)]
        s = turn(w, AT)
        a, b = (w, s) if f % 2 == 0 else (s, w)
        lines.append((pair(a[0:1], b[1:2]), a[2:3]))
    x0, x1 = (jnp.concatenate([line[i] for line in lines], axis=0) for i in range(2))

    d = dens[...].astype(f32)
    energy = jnp.sum(d * terms[...].astype(f32))
    dd = jnp.concatenate([d, d], axis=1)
    row, half = iota(dd.shape, 0), iota(dd.shape, 1) // AT
    diag = jnp.concatenate(
        [jnp.where(row == 2 * j + half, dd, 0.0).astype(bf16) for j in range(SLOTS // 2)], axis=1
    )

    copies[-1].wait()
    g0, g1, g2 = (dot(diag, ints[:, c].reshape(SLOTS * AT, 2 * AT)) for c in range(3))
    v0 = jnp.concatenate([pair(g0, turn(g1, AT)), pair(turn(g0, AT), g1)], axis=0)
    v1 = jnp.concatenate([g2, turn(g2, AT)], axis=0)

    lane = iota((2 * SLOTS, W), 1)
    shares = []
    for y in range(Y):
        rows = [
            jnp.where(lane == PLACE + r, place, window(v0, v1, Q * y, Q, Q * r)) for r in range(2)
        ]
        shares.append(jnp.concatenate(rows, axis=0))
    hi, lo = split(jnp.concatenate(shares, axis=1))
    sent = dot(route, hi) + dot(route, lo)
    at = iota((2 * 8, W), 1)
    for y in range(Y):
        extra = jnp.concatenate(
            [window(x0, x1, Q * y + Q // 2 * h, Q // 2, POS) for h in range(2)], axis=0
        )
        extra = jnp.where(at == SCALAR, energy, extra)
        share = sent[:, W * y : W * (y + 1)].reshape(XC, Z, W)
        for k in range(XC):
            out[k * Y + YS.index(y)] = jnp.where(at < POS, share[k], extra)


def me():
    return ((lax.axis_index("x") - X0) & (X - 1)) * C + (lax.axis_index("c") ^ C0)


def turn_kernel(got, out, pos):
    for k in range(XC):
        s = (got[k * Y] + got[k * Y + 1]) + (got[k * Y + 2] + got[k * Y + 3])
        out[:, k, :] = s
    mine = [got[me() * Y + YS.index(y)] for y in range(Y)]
    a = jnp.concatenate([m[:8] for m in mine], axis=0)
    b = jnp.concatenate([m[8:] for m in mine], axis=0)
    a, b = turn(a, -POS), turn(b, Q // 2 - POS)
    lane = iota(a.shape, 1)
    pos[...] = jnp.where(lane < Q // 2, a, jnp.where(lane < Q, b, 0.0))


def block_kernel(got, pos, out):
    v = got[...].reshape(Z * XC, W)
    lane = iota(v.shape, 1)
    f = iota((Z * XC, SLOTS), 1).astype(f32) * Y
    picks, datas = [], []
    for r in range(2):
        picks.append((v[:, PLACE + r : PLACE + r + 1] == f).astype(f32).astype(bf16))
        datas.append(jnp.where(lane < Q, turn(v, -Q * r), 0.0))
    pick = jnp.concatenate(picks, axis=0)
    hi, lo = split(jnp.concatenate(datas, axis=0))
    block = dot(pick, hi, ((0,), (0,))) + dot(pick, lo, ((0,), (0,)))
    virial = -jnp.sum(block * pos[...]) / 3.0
    energy = jnp.sum(jnp.where(lane == SCALAR, v, 0.0)) / (Z * PLANE)
    at = iota(block.shape, 1)
    block = jnp.where(at == SCALAR, energy, jnp.where(at == SCALAR - 1, virial, block))
    for k in range(PLANE):
        y = YS[k % Y]
        out[k] = block[8 * y : 8 * (y + 1)]


def force_kernel(got, forces, scalars):
    total = jnp.sum(got[:, 0:1, :], axis=0)
    scalars[...] = jnp.broadcast_to(total[None], scalars.shape)
    mine = [got[me() * Y + YS.index(y)] for y in range(Y)]
    lane = iota((8, W), 1)
    m1, m2 = turn(mine[1], Q), turn(mine[2], 2 * Q)
    u = jnp.where(lane < Q, mine[0], jnp.where(lane < 2 * Q, m1, m2))
    w = jnp.where(lane < 3 * Q - W, m2, turn(mine[3], 3 * Q - W))
    su, sw = turn(u, AT), turn(w, AT)
    for k in range(4):
        a, b = slice(2 * k, 2 * k + 1), slice(2 * k + 1, 2 * k + 2)
        cols = slice(W * k, W * (k + 1))
        forces[0:1, cols] = pair(u[a], su[b])
        forces[1:2, cols] = pair(su[a], u[b])
        forces[2:3, cols] = pair(w[a], sw[b])


VM = pl.BlockSpec(memory_space=pltpu.VMEM)
HBM = pl.BlockSpec(memory_space=pltpu.HBM)


def call(kernel, outs, n, scratch=(), where=VM):
    return pl.pallas_call(
        kernel,
        out_shape=outs,
        in_specs=[where] * n,
        out_specs=jax.tree.map(lambda _: VM, outs),
        scratch_shapes=scratch,
        compiler_params=pltpu.CompilerParams(vmem_limit_bytes=16 << 20),
    )


def arr(*shape):
    return jax.ShapeDtypeStruct(shape, f32)


def over_z(v):
    return lax.all_to_all(v, "z", 0, 0, axis_index_groups=[ZS], tiled=True)


def over_plane(v):
    order = [xc * Y + y for xc in XCS for y in YS]
    return lax.all_to_all(v, ("x", "c", "y"), 0, 0, axis_index_groups=[order], tiled=True)


def on_device(integrals, density, energy_terms, positions, dimer_owners, dimer_local):
    args = (
        jnp.transpose(integrals, (0, 2, 1, 3)),
        density,
        energy_terms,
        dimer_owners.T,
        dimer_local.T,
        positions,
    )
    scratch = [pltpu.VMEM(a.shape, a.dtype) for a in args] + [pltpu.SemaphoreType.DMA((6,))]
    args = (pltpu.with_memory_space_constraint(a, pltpu.HBM) for a in args)
    v = call(send_kernel, arr(PLANE, Z, W), 6, scratch, HBM)(*args)
    v = over_plane(v)
    v, pos = call(turn_kernel, (arr(Z, XC, W), arr(SLOTS, W)), 1)(v)
    v = over_z(v)
    v = call(block_kernel, arr(PLANE, 8, W), 2)(v, pos)
    v = over_plane(v)
    forces, v = call(force_kernel, (arr(3, 8 * AT), arr(Z, 1, W)), 1)(v)
    totals = jnp.sum(over_z(v), axis=(0, 1))
    return forces, totals[SCALAR], totals[SCALAR - 1]


def solution(mesh):
    split_mesh = Mesh(mesh.devices.reshape(X, Z, C, Y), ALL)
    placed = (
        P(DIMER, "y", None, None),
        P(DIMER, "y"),
        P(DIMER, "y"),
        P(None, ALL),
        P(DIMER, None),
        P(DIMER, None),
    )
    return jax.shard_map(
        on_device,
        mesh=split_mesh,
        in_specs=placed,
        out_specs=(P(None, ALL), P(), P()),
        check_vma=False,
    )
```

```python
import jax
import jax.numpy as jnp
from jax import lax
from jax.experimental import pallas as pl
from jax.experimental.pallas import tpu as pltpu
from jax.sharding import Mesh
from jax.sharding import PartitionSpec as P

X, Z, C, Y = 4, 16, 2, 4
XC = X * C
PLANE = XC * Y
AT = 64
W = 128
SLOTS = 32
Q = 48
PARTS = 4
PLACE, POS, SCALAR = 2 * Q, 98, 127
X0, C0, Y0, Z0 = 2, 1, 2, 8
ZS = [(Z0 + k) % Z for k in range(Z)]
YS = [(Y0 + k) % Y for k in range(Y)]
XCS = [(X0 + i) % X * C + (C0 + j) % C for i in range(X) for j in range(C)]
DIMER = ("x", "z", "c")
ALL = ("x", "z", "c", "y")
f32, bf16, i32 = jnp.float32, jnp.bfloat16, jnp.int32


def iota(shape, dim):
    return lax.broadcasted_iota(i32, shape, dim)


def split(v):
    hi = v.astype(bf16)
    return hi, (v - hi.astype(f32)).astype(bf16)


def dot(a, b, dims=((1,), (0,))):
    return lax.dot_general(a, b, (dims, ((), ())), preferred_element_type=f32)


def turn(v, by):
    by %= W
    return pltpu.roll(v, by, 1) if by else v


def pair(a, b):
    return jnp.where(iota(a.shape, 1) < AT, a, b)


def window(v0, v1, first, count, to):
    lane = iota(v0.shape, 1)
    inside = (lane >= to) & (lane < to + count)
    if first + count <= W:
        v = turn(v0, to - first)
    elif first >= W:
        v = turn(v1, to - first)
    else:
        v = jnp.where(lane < to + W - first, turn(v0, to - first), turn(v1, to - first))
    return jnp.where(inside, v, 0.0)


def send_kernel(h_ints, h_dens, h_terms, h_own, h_loc, h_pos, out, *scratch):
    ints, dens, terms, own, loc, pos, sems = scratch
    part = SLOTS // PARTS
    pairs = [(h_dens, dens), (h_own, own), (h_loc, loc), (h_pos, pos), (h_terms, terms)]
    pairs += [(h_ints.at[pl.ds(part * i, part)], ints.at[pl.ds(part * i, part)]) for i in range(PARTS)]
    copies = [pltpu.make_async_copy(a, b, sems.at[i]) for i, (a, b) in enumerate(pairs)]
    for copy in copies:
        copy.start()
    for copy in copies[:-PARTS]:
        copy.wait()

    o = jnp.concatenate([own[0:1], own[1:2]] * 2, axis=1)
    z = ((o >> 1) - Z0) & (Z - 1)
    xc = (((o >> 5) - X0) & (X - 1)) * C + ((o & 1) ^ C0)
    e = (iota((XC * Z, W), 0) == xc * Z + z).astype(f32).astype(bf16)
    p, q = iota((W, W), 0), iota((W, W), 1)
    before = ((p < 2 * SLOTS) & (p < q % (2 * SLOTS))).astype(f32).astype(bf16)
    count = dot(e, before)
    rank = (iota((XC * Z, W), 1) >= 2 * SLOTS).astype(f32)
    route = jnp.where(count == rank, e.astype(f32), 0.0).astype(bf16)
    same = iota((SLOTS, SLOTS), 0) == iota((SLOTS, SLOTS), 1)
    places = [
        jnp.sum(jnp.where(same, loc[t : t + 1].astype(f32), 0.0), axis=1, keepdims=True)
        for t in range(2)
    ]
    place = jnp.concatenate([jnp.broadcast_to(v, (SLOTS, W)) for v in places], axis=0)

    lines = []
    for f in range(8):
        w = pos[:, W * (f // 2) : W * (f // 2 + 1)]
        s = turn(w, AT)
        a, b = (w, s) if f % 2 == 0 else (s, w)
        lines.append((pair(a[0:1], b[1:2]), a[2:3]))
    x0, x1 = (jnp.concatenate([line[i] for line in lines], axis=0) for i in range(2))

    d = dens[...].astype(f32)
    energy = jnp.sum(d * terms[...].astype(f32))
    dd = jnp.concatenate([d, d], axis=1)
    row, half = iota(dd.shape, 0), iota(dd.shape, 1) // AT
    diag = jnp.concatenate(
        [jnp.where(row == 2 * j + half, dd, 0.0).astype(bf16) for j in range(SLOTS // 2)], axis=1
    )

    g = jnp.zeros((SLOTS, 3 * W), f32)
    for i in range(PARTS):
        copies[i - PARTS].wait()
        rows = [ints[pl.ds(part * i, part), c].reshape(part * AT, W) for c in range(3)]
        g += dot(diag[:, part * AT * i : part * AT * (i + 1)], jnp.concatenate(rows, axis=1))
    g0, g1, g2 = (g[:, W * c : W * (c + 1)] for c in range(3))
    v0 = jnp.concatenate([pair(g0, turn(g1, AT)), pair(turn(g0, AT), g1)], axis=0)
    v1 = jnp.concatenate([g2, turn(g2, AT)], axis=0)

    lane = iota((2 * SLOTS, W), 1)
    shares = []
    for y in range(Y):
        rows = [
            jnp.where(lane == PLACE + r, place, window(v0, v1, Q * y, Q, Q * r)) for r in range(2)
        ]
        shares.append(jnp.concatenate(rows, axis=0))
    hi, lo = split(jnp.concatenate(shares, axis=1))
    sent = dot(route, hi) + dot(route, lo)
    at = iota((2 * 8, W), 1)
    for y in range(Y):
        extra = jnp.concatenate(
            [window(x0, x1, Q * y + Q // 2 * h, Q // 2, POS) for h in range(2)], axis=0
        )
        extra = jnp.where(at == SCALAR, energy, extra)
        share = sent[:, W * y : W * (y + 1)].reshape(XC, Z, W)
        for k in range(XC):
            out[k * Y + YS.index(y)] = jnp.where(at < POS, share[k], extra)


def me():
    return ((lax.axis_index("x") - X0) & (X - 1)) * C + (lax.axis_index("c") ^ C0)


def turn_kernel(got, out, pos):
    for k in range(XC):
        s = (got[k * Y] + got[k * Y + 1]) + (got[k * Y + 2] + got[k * Y + 3])
        out[:, k, :] = s
    mine = [got[me() * Y + YS.index(y)] for y in range(Y)]
    a = jnp.concatenate([m[:8] for m in mine], axis=0)
    b = jnp.concatenate([m[8:] for m in mine], axis=0)
    a, b = turn(a, -POS), turn(b, Q // 2 - POS)
    lane = iota(a.shape, 1)
    pos[...] = jnp.where(lane < Q // 2, a, jnp.where(lane < Q, b, 0.0))


def block_kernel(got, pos, out):
    v = got[...].reshape(Z * XC, W)
    lane = iota(v.shape, 1)
    f = iota((Z * XC, SLOTS), 1).astype(f32) * Y
    picks, datas = [], []
    for r in range(2):
        picks.append((v[:, PLACE + r : PLACE + r + 1] == f).astype(f32).astype(bf16))
        datas.append(jnp.where(lane < Q, turn(v, -Q * r), 0.0))
    pick = jnp.concatenate(picks, axis=0)
    hi, lo = split(jnp.concatenate(datas, axis=0))
    block = dot(pick, hi, ((0,), (0,))) + dot(pick, lo, ((0,), (0,)))
    virial = -jnp.sum(block * pos[...]) / 3.0
    energy = jnp.sum(jnp.where(lane == SCALAR, v, 0.0)) / (Z * PLANE)
    at = iota(block.shape, 1)
    block = jnp.where(at == SCALAR, energy, jnp.where(at == SCALAR - 1, virial, block))
    lower = turn(pltpu.roll(block, SLOTS - 4, 0), Q)
    block = jnp.where((at < Q) | (at >= 2 * Q), block, lower)
    for k in range(PLANE):
        y = YS[k % Y]
        out[k] = block[8 * y : 8 * y + 4]


def scalar_kernel(got, scalars):
    total = jnp.sum(got[:, 0:1, :], axis=0)
    scalars[...] = jnp.broadcast_to(total[None], scalars.shape)


def force_kernel(got, scalars, forces, energy, virial):
    total = jnp.sum(scalars[...], axis=0)
    energy[0] = total[0, SCALAR]
    virial[0] = total[0, SCALAR - 1]
    mine = [got[me() * Y + YS.index(y)] for y in range(Y)]
    mine = [jnp.concatenate([m, turn(m, -Q)], axis=0) for m in mine]
    lane = iota((8, W), 1)
    m1, m2 = turn(mine[1], Q), turn(mine[2], 2 * Q)
    u = jnp.where(lane < Q, mine[0], jnp.where(lane < 2 * Q, m1, m2))
    w = jnp.where(lane < 3 * Q - W, m2, turn(mine[3], 3 * Q - W))
    su, sw = turn(u, AT), turn(w, AT)
    for k in range(4):
        a, b = slice(2 * k, 2 * k + 1), slice(2 * k + 1, 2 * k + 2)
        cols = slice(W * k, W * (k + 1))
        forces[0:1, cols] = pair(u[a], su[b])
        forces[1:2, cols] = pair(su[a], u[b])
        forces[2:3, cols] = pair(w[a], sw[b])


VM = pl.BlockSpec(memory_space=pltpu.VMEM)
HBM = pl.BlockSpec(memory_space=pltpu.HBM)
SM = pl.BlockSpec(memory_space=pltpu.SMEM)


def call(kernel, outs, n, scratch=(), where=VM, spaces=None):
    return pl.pallas_call(
        kernel,
        out_shape=outs,
        in_specs=[where] * n,
        out_specs=spaces or jax.tree.map(lambda _: VM, outs),
        scratch_shapes=scratch,
        cost_estimate=pl.CostEstimate(flops=20_000_000, bytes_accessed=1 << 18, transcendentals=0),
        compiler_params=pltpu.CompilerParams(vmem_limit_bytes=16 << 20),
    )


def arr(*shape):
    return jax.ShapeDtypeStruct(shape, f32)


def over_z(v):
    return lax.all_to_all(v, "z", 0, 0, axis_index_groups=[ZS], tiled=True)


def over_plane(v):
    order = [xc * Y + y for xc in XCS for y in YS]
    return lax.all_to_all(v, ("x", "c", "y"), 0, 0, axis_index_groups=[order], tiled=True)


def on_device(integrals, density, energy_terms, positions, dimer_owners, dimer_local):
    args = (
        jnp.transpose(integrals, (0, 2, 1, 3)),
        density,
        energy_terms,
        dimer_owners.T,
        dimer_local.T,
        positions,
    )
    scratch = [pltpu.VMEM(a.shape, a.dtype) for a in args] + [pltpu.SemaphoreType.DMA((5 + PARTS,))]
    args = (pltpu.with_memory_space_constraint(a, pltpu.HBM) for a in args)
    v = call(send_kernel, arr(PLANE, Z, W), 6, scratch, HBM)(*args)
    v = over_plane(v)
    v, pos = call(turn_kernel, (arr(Z, XC, W), arr(SLOTS, W)), 1)(v)
    v = over_z(v)
    v = call(block_kernel, arr(PLANE, 4, W), 2)(v, pos)
    v = over_plane(v)
    scalars = over_z(call(scalar_kernel, arr(Z, 1, W), 1)(v))
    outs = (arr(3, 8 * AT), arr(1), arr(1))
    forces, energy, virial = call(force_kernel, outs, 2, spaces=(VM, SM, SM))(v, scalars)
    return forces, energy.reshape(()), virial.reshape(())


def solution(mesh):
    split_mesh = Mesh(mesh.devices.reshape(X, Z, C, Y), ALL)
    placed = (
        P(DIMER, "y", None, None),
        P(DIMER, "y"),
        P(DIMER, "y"),
        P(None, ALL),
        P(DIMER, None),
        P(DIMER, None),
    )
    return jax.shard_map(
        on_device,
        mesh=split_mesh,
        in_specs=placed,
        out_specs=(P(None, ALL), P(), P()),
        check_vma=False,
    )
```

```python
import jax
import jax.numpy as jnp
from jax import lax
from jax.experimental import pallas as pl
from jax.experimental.pallas import tpu as pltpu
from jax.sharding import Mesh
from jax.sharding import PartitionSpec as P

X, Z, C, Y = 4, 16, 2, 4
XC = X * C
PLANE = XC * Y
AT = 64
W = 128
SLOTS = 32
Q = 48
PARTS = 4
PLACE, SCALAR = Q, 127
X0, C0, Y0, Z0 = 2, 1, 2, 8
ZS = [(Z0 + k) % Z for k in range(Z)]
YS = [(Y0 + k) % Y for k in range(Y)]
XCS = [(X0 + i) % X * C + (C0 + j) % C for i in range(X) for j in range(C)]
DIMER = ("x", "z", "c")
ALL = ("x", "z", "c", "y")
f32, bf16, i32 = jnp.float32, jnp.bfloat16, jnp.int32


def iota(shape, dim):
    return lax.broadcasted_iota(i32, shape, dim)


def split(v):
    hi = v.astype(bf16)
    return hi, (v - hi.astype(f32)).astype(bf16)


def dot(a, b, dims=((1,), (0,))):
    return lax.dot_general(a, b, (dims, ((), ())), preferred_element_type=f32)


def turn(v, by):
    by %= W
    return pltpu.roll(v, by, 1) if by else v


def pair(a, b):
    return jnp.where(iota(a.shape, 1) < AT, a, b)


def window(v0, v1, first, count, to):
    lane = iota(v0.shape, 1)
    inside = (lane >= to) & (lane < to + count)
    if first + count <= W:
        v = turn(v0, to - first)
    elif first >= W:
        v = turn(v1, to - first)
    else:
        v = jnp.where(lane < to + W - first, turn(v0, to - first), turn(v1, to - first))
    return jnp.where(inside, v, 0.0)


def send_kernel(h_ints, h_dens, h_terms, h_own, h_loc, h_pos, out, *scratch):
    ints, dens, terms, own, loc, pos, sems = scratch
    part = SLOTS // PARTS
    pairs = [(h_dens, dens), (h_own, own), (h_loc, loc), (h_pos, pos), (h_terms, terms)]
    pairs += [(h_ints.at[pl.ds(part * i, part)], ints.at[pl.ds(part * i, part)]) for i in range(PARTS)]
    copies = [pltpu.make_async_copy(a, b, sems.at[i]) for i, (a, b) in enumerate(pairs)]
    for copy in copies:
        copy.start()
    for copy in copies[:-PARTS]:
        copy.wait()

    o = jnp.concatenate([own[0:1], own[1:2]] * 2, axis=1)
    f = jnp.concatenate([loc[0:1], loc[1:2]] * 2, axis=1)
    z = ((o >> 1) - Z0) & (Z - 1)
    xc = (((o >> 5) - X0) & (X - 1)) * C + ((o & 1) ^ C0)
    f = ((((f >> 3) - Y0) & (Y - 1)) << 3) + (f & 7)
    row, col = iota((2 * SLOTS, W), 0), iota((2 * SLOTS, W), 1)
    key = ((z * 8 + xc) * SLOTS + f) * (2 * SLOTS) + (col[:1] & (2 * SLOTS - 1))
    key_of = jnp.sum(jnp.where(row == col, key.astype(f32), 0.0), axis=1, keepdims=True)
    turn_of = jnp.sum((key_of < key.astype(f32)).astype(f32), axis=0, keepdims=True).astype(i32)
    route = (row == (turn_of & 7) * 8 + (turn_of >> 3)).astype(f32).astype(bf16)
    place = (key_of.astype(i32) >> 6).astype(f32)

    lines = []
    for f in range(8):
        w = pos[:, W * (f // 2) : W * (f // 2 + 1)]
        s = turn(w, AT)
        a, b = (w, s) if f % 2 == 0 else (s, w)
        lines.append((pair(a[0:1], b[1:2]), a[2:3]))
    x0, x1 = (jnp.concatenate([line[i] for line in lines], axis=0) for i in range(2))

    d = dens[...].astype(f32)
    energy = jnp.sum(d * terms[...].astype(f32))
    dd = jnp.concatenate([d, d], axis=1)
    row, half = iota(dd.shape, 0), iota(dd.shape, 1) // AT
    diag = jnp.concatenate(
        [jnp.where(row == 2 * j + half, dd, 0.0).astype(bf16) for j in range(SLOTS // 2)], axis=1
    )

    for copy in copies[-PARTS:]:
        copy.wait()
    g0, g1, g2 = (dot(diag, ints[:, c].reshape(SLOTS * AT, W)) for c in range(3))
    v0 = jnp.concatenate([pair(g0, turn(g1, AT)), pair(turn(g0, AT), g1)], axis=0)
    v1 = jnp.concatenate([g2, turn(g2, AT)], axis=0)

    shares = [jnp.where(col == PLACE, place, window(v0, v1, Q * y, Q, 0)) for y in range(Y)]
    sent = dot(route, jnp.concatenate(split(jnp.concatenate(shares, axis=1)), axis=0))
    at = iota((8, W), 1)
    for y in range(Y):
        extra = jnp.where(at == SCALAR, energy, window(x0, x1, Q * y, Q, AT))
        for k in range(XC):
            share = sent[8 * k : 8 * (k + 1), W * y : W * (y + 1)]
            out[k * Y + YS.index(y)] = pair(share, extra)


def turn_kernel(got, out):
    s = jnp.concatenate(
        [
            (got[k * Y] + got[k * Y + 1]) + (got[k * Y + 2] + got[k * Y + 3])
            for k in range(XC)
        ],
        axis=0,
    )
    row, col = iota(s.shape, 0), iota(s.shape, 1)
    place = s[:, PLACE : PLACE + 1].astype(i32)
    z, place = place >> 10, (place & 1023).astype(f32)
    e = (((row >> 3) == (col & 7)) & (z == (col >> 3))).astype(f32)
    before = (iota((64, 64), 1) < iota((64, 64), 0)).astype(f32).astype(bf16)
    count = dot(before, e.astype(bf16))
    route = jnp.concatenate([jnp.where(count == r, e, 0.0) for r in (0.0, 1.0)], axis=0)
    route = route.astype(bf16)
    low = jnp.where(col < Q, s, jnp.where(col == PLACE, place, 0.0))
    hi, lo = split(jnp.concatenate([low, turn(low, AT)], axis=0))
    v = dot(route, hi, ((0,), (0,))) + dot(route, lo, ((0,), (0,)))
    energy = jnp.sum(jnp.where((row & 7) == 0, s, 0.0), axis=0, keepdims=True)
    v = jnp.where(iota(v.shape, 1) == SCALAR, energy, v)
    out[...] = v.reshape(Z, XC, W)


def block_kernel(got, first, out):
    v = got[...].reshape(Z * XC, W)
    row, col = iota(v.shape, 0), iota(v.shape, 1)
    upper = (col >= AT) & (col < AT + Q)
    f = iota((Z * XC, PLANE * 8), 1).astype(f32) * Y
    picks = [(v[:, p : p + 1] == f).astype(f32).astype(bf16) for p in (PLACE, AT + PLACE)]
    pick = jnp.concatenate(picks, axis=0)
    data = jnp.concatenate([jnp.where(upper, d, 0.0) for d in (turn(v, AT), v)], axis=0)
    hi, lo = split(data)
    block = dot(pick, hi, ((0,), (0,))) + dot(pick, lo, ((0,), (0,)))
    virial = -jnp.sum(block * first[...].reshape(block.shape)) / 3.0
    energy = jnp.sum(jnp.where(((row & 7) == 0) & (col == SCALAR), v, 0.0)) / (Z * PLANE)
    at = iota(block.shape, 1)
    lower = turn(pltpu.roll(block, PLANE * 8 - 4, 0), -Q)
    block = jnp.where(at < AT, lower, block)
    block = jnp.where(at == SCALAR, energy, jnp.where(at == SCALAR - 1, virial, block))
    for k in range(PLANE):
        out[k] = block[8 * k : 8 * k + 4]


def scalar_kernel(got, scalars):
    total = jnp.sum(got[:, 0:1, :], axis=0)
    scalars[...] = jnp.broadcast_to(total[None], scalars.shape)


def force_kernel(got, scalars, forces, energy, virial):
    total = jnp.sum(scalars[...], axis=0)
    energy[0] = total[0, SCALAR]
    virial[0] = total[0, SCALAR - 1]
    mine = [sum(got[k * Y + YS.index(y)] for k in range(XC)) for y in range(Y)]
    mine = [jnp.concatenate([turn(m, -AT), turn(m, Q - AT)], axis=0) for m in mine]
    lane = iota((8, W), 1)
    m1, m2 = turn(mine[1], Q), turn(mine[2], 2 * Q)
    u = jnp.where(lane < Q, mine[0], jnp.where(lane < 2 * Q, m1, m2))
    w = jnp.where(lane < 3 * Q - W, m2, turn(mine[3], 3 * Q - W))
    su, sw = turn(u, AT), turn(w, AT)
    for k in range(4):
        a, b = slice(2 * k, 2 * k + 1), slice(2 * k + 1, 2 * k + 2)
        cols = slice(W * k, W * (k + 1))
        forces[0:1, cols] = pair(u[a], su[b])
        forces[1:2, cols] = pair(su[a], u[b])
        forces[2:3, cols] = pair(w[a], sw[b])


VM = pl.BlockSpec(memory_space=pltpu.VMEM)
HBM = pl.BlockSpec(memory_space=pltpu.HBM)
SM = pl.BlockSpec(memory_space=pltpu.SMEM)


def call(kernel, outs, n, scratch=(), where=VM, spaces=None):
    return pl.pallas_call(
        kernel,
        out_shape=outs,
        in_specs=[where] * n,
        out_specs=spaces or jax.tree.map(lambda _: VM, outs),
        scratch_shapes=scratch,
        cost_estimate=pl.CostEstimate(flops=20_000_000, bytes_accessed=1 << 18, transcendentals=0),
        compiler_params=pltpu.CompilerParams(vmem_limit_bytes=16 << 20),
    )


def arr(*shape):
    return jax.ShapeDtypeStruct(shape, f32)


def over_z(v):
    return lax.all_to_all(v, "z", 0, 0, axis_index_groups=[ZS], tiled=True)


def over_plane(v):
    order = [xc * Y + y for xc in XCS for y in YS]
    return lax.all_to_all(v, ("x", "c", "y"), 0, 0, axis_index_groups=[order], tiled=True)


def on_device(integrals, density, energy_terms, positions, dimer_owners, dimer_local):
    args = (
        jnp.transpose(integrals, (0, 2, 1, 3)),
        density,
        energy_terms,
        dimer_owners.T,
        dimer_local.T,
        positions,
    )
    scratch = [pltpu.VMEM(a.shape, a.dtype) for a in args] + [pltpu.SemaphoreType.DMA((5 + PARTS,))]
    args = (pltpu.with_memory_space_constraint(a, pltpu.HBM) for a in args)
    first = over_plane(call(send_kernel, arr(PLANE, 8, W), 6, scratch, HBM)(*args))
    v = over_z(call(turn_kernel, arr(Z, XC, W), 1)(first))
    v = call(block_kernel, arr(PLANE, 4, W), 2)(v, first)
    v = over_plane(v)
    scalars = over_z(call(scalar_kernel, arr(Z, 1, W), 1)(v))
    outs = (arr(3, 8 * AT), arr(1), arr(1))
    forces, energy, virial = call(force_kernel, outs, 2, spaces=(VM, SM, SM))(v, scalars)
    return forces, energy.reshape(()), virial.reshape(())


def solution(mesh):
    split_mesh = Mesh(mesh.devices.reshape(X, Z, C, Y), ALL)
    placed = (
        P(DIMER, "y", None, None),
        P(DIMER, "y"),
        P(DIMER, "y"),
        P(None, ALL),
        P(DIMER, None),
        P(DIMER, None),
    )
    return jax.shard_map(
        on_device,
        mesh=split_mesh,
        in_specs=placed,
        out_specs=(P(None, ALL), P(), P()),
        check_vma=False,
    )
```

```python
import jax
import jax.numpy as jnp
from jax import lax
from jax.experimental import pallas as pl
from jax.experimental.pallas import tpu as pltpu
from jax.sharding import Mesh
from jax.sharding import PartitionSpec as P

X, Z, C, Y = 4, 16, 2, 4
XC = X * C
PLANE = XC * Y
AT = 64
W = 128
SLOTS = 32
Q = 48
PARTS = 4
PLACE, SCALAR = Q, 127
X0, C0, Y0, Z0 = 2, 1, 2, 8
ZS = [(Z0 + k) % Z for k in range(Z)]
YS = [(Y0 + k) % Y for k in range(Y)]
XCS = [(X0 + i) % X * C + (C0 + j) % C for i in range(X) for j in range(C)]
DIMER = ("x", "z", "c")
ALL = ("x", "z", "c", "y")
f32, bf16, i32 = jnp.float32, jnp.bfloat16, jnp.int32


def iota(shape, dim):
    return lax.broadcasted_iota(i32, shape, dim)


def split(v):
    hi = v.astype(bf16)
    return hi, (v - hi.astype(f32)).astype(bf16)


def dot(a, b, dims=((1,), (0,))):
    return lax.dot_general(a, b, (dims, ((), ())), preferred_element_type=f32)


def turn(v, by):
    by %= W
    return pltpu.roll(v, by, 1) if by else v


def pair(a, b):
    return jnp.where(iota(a.shape, 1) < AT, a, b)


def window(v0, v1, first, count, to):
    lane = iota(v0.shape, 1)
    inside = (lane >= to) & (lane < to + count)
    if first + count <= W:
        v = turn(v0, to - first)
    elif first >= W:
        v = turn(v1, to - first)
    else:
        v = jnp.where(lane < to + W - first, turn(v0, to - first), turn(v1, to - first))
    return jnp.where(inside, v, 0.0)


def send_kernel(h_ints, h_dens, h_terms, h_own, h_loc, h_pos, out, *scratch):
    ints, dens, terms, own, loc, pos, sems = scratch
    part = SLOTS // PARTS
    pairs = [(h_dens, dens), (h_own, own), (h_loc, loc), (h_pos, pos), (h_terms, terms)]
    pairs += [(h_ints.at[pl.ds(part * i, part)], ints.at[pl.ds(part * i, part)]) for i in range(PARTS)]
    copies = [pltpu.make_async_copy(a, b, sems.at[i]) for i, (a, b) in enumerate(pairs)]
    for copy in copies:
        copy.start()
    for copy in copies[:-PARTS]:
        copy.wait()

    o = jnp.concatenate([own[0:1], own[1:2]] * 2, axis=1)
    f = jnp.concatenate([loc[0:1], loc[1:2]] * 2, axis=1)
    z = ((o >> 1) - Z0) & (Z - 1)
    xc = (((o >> 5) - X0) & (X - 1)) * C + ((o & 1) ^ C0)
    f = ((((f >> 3) - Y0) & (Y - 1)) << 3) + (f & 7)
    row, col = iota((2 * SLOTS, W), 0), iota((2 * SLOTS, W), 1)
    key = ((z * 8 + xc) * SLOTS + f) * (2 * SLOTS) + (col[:1] & (2 * SLOTS - 1))
    key_of = jnp.sum(jnp.where(row == col, key.astype(f32), 0.0), axis=1, keepdims=True)
    turn_of = jnp.sum((key_of < key.astype(f32)).astype(f32), axis=0, keepdims=True).astype(i32)
    chosen = (row == (turn_of & 7) * 8 + (turn_of >> 3)) & (col < 2 * SLOTS)
    place = jnp.sum(jnp.where(chosen, (key >> 6).astype(f32), 0.0), axis=1, keepdims=True)
    second = jnp.sum(jnp.where(chosen & (col >= SLOTS), 1.0, 0.0), axis=1, keepdims=True) > 0

    lines = []
    for f in range(8):
        w = pos[:, W * (f // 2) : W * (f // 2 + 1)]
        s = turn(w, AT)
        a, b = (w, s) if f % 2 == 0 else (s, w)
        lines.append((pair(a[0:1], b[1:2]), a[2:3]))
    x0, x1 = (jnp.concatenate([line[i] for line in lines], axis=0) for i in range(2))

    d = dens[...].astype(f32)
    energy = jnp.sum(d * terms[...].astype(f32))
    dd = jnp.concatenate([d, d], axis=1)
    side, half = iota(dd.shape, 0), iota(dd.shape, 1) // AT
    diag = jnp.concatenate(
        [jnp.where(side == 2 * j + half, dd, 0.0).astype(bf16) for j in range(SLOTS // 2)], axis=1
    )
    route = chosen.astype(f32).astype(bf16)[:, : 2 * SLOTS]
    weights = dot(route, jnp.concatenate([diag, diag], axis=0)).astype(bf16)

    for copy in copies[-PARTS:]:
        copy.wait()
    g = [dot(weights, ints[:, c].reshape(SLOTS * AT, W)) for c in range(3)]
    h = [turn(v, AT) for v in g]
    v0 = pair(jnp.where(second, h[0], g[0]), jnp.where(second, g[1], h[1]))
    v1 = jnp.where(second, h[2], g[2])
    shares = [jnp.where(col == PLACE, place, window(v0, v1, Q * y, Q, 0)) for y in range(Y)]
    at = iota((8, W), 1)
    for y in range(Y):
        extra = jnp.where(at == SCALAR, energy, window(x0, x1, Q * y, Q, AT))
        for k in range(XC):
            out[k * Y + YS.index(y)] = pair(shares[y][8 * k : 8 * (k + 1)], extra)


def turn_kernel(got, out):
    s = jnp.concatenate(
        [
            (got[k * Y] + got[k * Y + 1]) + (got[k * Y + 2] + got[k * Y + 3])
            for k in range(XC)
        ],
        axis=0,
    )
    row, col = iota(s.shape, 0), iota(s.shape, 1)
    place = s[:, PLACE : PLACE + 1].astype(i32)
    z, place = place >> 10, (place & 1023).astype(f32)
    e = ((row >> 3) == (col & 7)) & (z == (col >> 3))
    z = jnp.broadcast_to(z, s.shape)
    again = (z == pltpu.roll(z, 1, 0)) & ((row & 7) != 0)
    route = jnp.concatenate([(e & ~again).astype(f32), (e & again).astype(f32)], axis=0)
    route = route.astype(bf16)
    low = jnp.where(col < Q, s, jnp.where(col == PLACE, place, 0.0))
    hi, lo = split(jnp.concatenate([low, turn(low, AT)], axis=0))
    v = dot(route, hi, ((0,), (0,))) + dot(route, lo, ((0,), (0,)))
    energy = jnp.sum(jnp.where((row & 7) == 0, s, 0.0), axis=0, keepdims=True)
    v = jnp.where(iota(v.shape, 1) == SCALAR, energy, v)
    out[...] = v.reshape(Z, XC, W)


def block_kernel(got, first, out):
    v = got[...].reshape(Z * XC, W)
    row, col = iota(v.shape, 0), iota(v.shape, 1)
    upper = (col >= AT) & (col < AT + Q)
    f = iota((Z * XC, PLANE * 8), 1).astype(f32) * Y
    picks = [(v[:, p : p + 1] == f).astype(f32).astype(bf16) for p in (PLACE, AT + PLACE)]
    pick = jnp.concatenate(picks, axis=0)
    data = jnp.concatenate([jnp.where(upper, d, 0.0) for d in (turn(v, AT), v)], axis=0)
    hi, lo = split(data)
    block = dot(pick, hi, ((0,), (0,))) + dot(pick, lo, ((0,), (0,)))
    virial = -jnp.sum(block * first[...].reshape(block.shape)) / 3.0
    energy = jnp.sum(jnp.where((row & 7) == 0, v, 0.0), axis=0, keepdims=True) / (Z * PLANE)
    at = iota(block.shape, 1)
    lower = turn(pltpu.roll(block, PLANE * 8 - 4, 0), -Q)
    block = jnp.where(at < AT, lower, block)
    block = jnp.where(at == SCALAR, energy, jnp.where(at == SCALAR - 1, virial, block))
    for k in range(PLANE):
        out[k] = block[8 * k : 8 * k + 4]


def scalar_kernel(got, scalars):
    total = jnp.sum(got[:, 0:1, :], axis=0)
    scalars[...] = jnp.broadcast_to(total[None], scalars.shape)


def force_kernel(got, scalars, forces, energy, virial):
    total = jnp.sum(scalars[...], axis=0)
    energy[0] = total[0, SCALAR]
    virial[0] = total[0, SCALAR - 1]
    mine = [sum(got[k * Y + YS.index(y)] for k in range(XC)) for y in range(Y)]
    mine = [jnp.concatenate([turn(m, -AT), turn(m, Q - AT)], axis=0) for m in mine]
    lane = iota((8, W), 1)
    m1, m2 = turn(mine[1], Q), turn(mine[2], 2 * Q)
    u = jnp.where(lane < Q, mine[0], jnp.where(lane < 2 * Q, m1, m2))
    w = jnp.where(lane < 3 * Q - W, m2, turn(mine[3], 3 * Q - W))
    su, sw = turn(u, AT), turn(w, AT)
    for k in range(4):
        a, b = slice(2 * k, 2 * k + 1), slice(2 * k + 1, 2 * k + 2)
        cols = slice(W * k, W * (k + 1))
        forces[0:1, cols] = pair(u[a], su[b])
        forces[1:2, cols] = pair(su[a], u[b])
        forces[2:3, cols] = pair(w[a], sw[b])


VM = pl.BlockSpec(memory_space=pltpu.VMEM)
HBM = pl.BlockSpec(memory_space=pltpu.HBM)
SM = pl.BlockSpec(memory_space=pltpu.SMEM)


def call(kernel, outs, n, scratch=(), where=VM, spaces=None):
    return pl.pallas_call(
        kernel,
        out_shape=outs,
        in_specs=[where] * n,
        out_specs=spaces or jax.tree.map(lambda _: VM, outs),
        scratch_shapes=scratch,
        cost_estimate=pl.CostEstimate(flops=20_000_000, bytes_accessed=1 << 18, transcendentals=0),
        compiler_params=pltpu.CompilerParams(vmem_limit_bytes=16 << 20),
    )


def arr(*shape):
    return jax.ShapeDtypeStruct(shape, f32)


def over_z(v):
    return lax.all_to_all(v, "z", 0, 0, axis_index_groups=[ZS], tiled=True)


def over_plane(v):
    order = [xc * Y + y for xc in XCS for y in YS]
    return lax.all_to_all(v, ("x", "c", "y"), 0, 0, axis_index_groups=[order], tiled=True)


def on_device(integrals, density, energy_terms, positions, dimer_owners, dimer_local):
    args = (
        jnp.transpose(integrals, (0, 2, 1, 3)),
        density,
        energy_terms,
        dimer_owners.T,
        dimer_local.T,
        positions,
    )
    scratch = [pltpu.VMEM(a.shape, a.dtype) for a in args] + [pltpu.SemaphoreType.DMA((5 + PARTS,))]
    args = (pltpu.with_memory_space_constraint(a, pltpu.HBM) for a in args)
    first = over_plane(call(send_kernel, arr(PLANE, 8, W), 6, scratch, HBM)(*args))
    v = over_z(call(turn_kernel, arr(Z, XC, W), 1)(first))
    v = call(block_kernel, arr(PLANE, 4, W), 2)(v, first)
    v = over_plane(v)
    scalars = over_z(call(scalar_kernel, arr(Z, 1, W), 1)(v))
    outs = (arr(3, 8 * AT), arr(1), arr(1))
    forces, energy, virial = call(force_kernel, outs, 2, spaces=(VM, SM, SM))(v, scalars)
    return forces, energy.reshape(()), virial.reshape(())


def solution(mesh):
    split_mesh = Mesh(mesh.devices.reshape(X, Z, C, Y), ALL)
    placed = (
        P(DIMER, "y", None, None),
        P(DIMER, "y"),
        P(DIMER, "y"),
        P(None, ALL),
        P(DIMER, None),
        P(DIMER, None),
    )
    return jax.shard_map(
        on_device,
        mesh=split_mesh,
        in_specs=placed,
        out_specs=(P(None, ALL), P(), P()),
        check_vma=False,
    )
```

```python
import jax
import jax.numpy as jnp
from jax import lax
from jax.experimental import pallas as pl
from jax.experimental.pallas import tpu as pltpu
from jax.sharding import Mesh
from jax.sharding import PartitionSpec as P

X, Z, C, Y = 4, 16, 2, 4
XC = X * C
PLANE = XC * Y
AT = 64
W = 128
SLOTS = 32
Q = 48
PARTS = 4
PLACE, SCALAR = Q, 127
X0, C0, Y0, Z0 = 2, 1, 2, 9
ZS = [(Z0 + k) % Z for k in range(Z)]
YS = [(Y0 + k) % Y for k in range(Y)]
XCS = [(X0 + i) % X * C + (C0 + j) % C for i in range(X) for j in range(C)]
DIMER = ("x", "z", "c")
ALL = ("x", "z", "c", "y")
f32, bf16, i32 = jnp.float32, jnp.bfloat16, jnp.int32


def iota(shape, dim):
    return lax.broadcasted_iota(i32, shape, dim)


def split(v):
    hi = v.astype(bf16)
    return hi, (v - hi.astype(f32)).astype(bf16)


def dot(a, b, dims=((1,), (0,))):
    return lax.dot_general(a, b, (dims, ((), ())), preferred_element_type=f32)


def turn(v, by):
    by %= W
    return pltpu.roll(v, by, 1) if by else v


def pair(a, b):
    return jnp.where(iota(a.shape, 1) < AT, a, b)


def window(v0, v1, first, count, to):
    lane = iota(v0.shape, 1)
    inside = (lane >= to) & (lane < to + count)
    if first + count <= W:
        v = turn(v0, to - first)
    elif first >= W:
        v = turn(v1, to - first)
    else:
        v = jnp.where(lane < to + W - first, turn(v0, to - first), turn(v1, to - first))
    return jnp.where(inside, v, 0.0)


def send_kernel(h_ints, h_dens, h_terms, h_own, h_loc, h_pos, out, *scratch):
    ints, dens, terms, own, loc, pos, sems = scratch
    part = SLOTS // PARTS
    pairs = [(h_dens, dens), (h_own, own), (h_loc, loc), (h_pos, pos), (h_terms, terms)]
    pairs += [(h_ints.at[pl.ds(part * i, part)], ints.at[pl.ds(part * i, part)]) for i in range(PARTS)]
    copies = [pltpu.make_async_copy(a, b, sems.at[i]) for i, (a, b) in enumerate(pairs)]
    for copy in copies:
        copy.start()
    for copy in copies[:-PARTS]:
        copy.wait()

    o = jnp.concatenate([own[0:1], own[1:2]] * 2, axis=1)
    f = jnp.concatenate([loc[0:1], loc[1:2]] * 2, axis=1)
    z = ((o >> 1) - Z0) & (Z - 1)
    xc = (((o >> 5) - X0) & (X - 1)) * C + ((o & 1) ^ C0)
    f = ((((f >> 3) - Y0) & (Y - 1)) << 3) + (f & 7)
    row, col = iota((2 * SLOTS, W), 0), iota((2 * SLOTS, W), 1)
    key = ((z * 8 + xc) * SLOTS + f) * (2 * SLOTS) + (col[:1] & (2 * SLOTS - 1))
    key_of = jnp.sum(jnp.where(row == col, key.astype(f32), 0.0), axis=1, keepdims=True)
    turn_of = jnp.sum((key_of < key.astype(f32)).astype(f32), axis=0, keepdims=True).astype(i32)
    chosen = (row == (turn_of & 7) * 8 + (turn_of >> 3)) & (col < 2 * SLOTS)
    place = jnp.sum(jnp.where(chosen, (key >> 6).astype(f32), 0.0), axis=1, keepdims=True)
    second = jnp.sum(jnp.where(chosen & (col >= SLOTS), 1.0, 0.0), axis=1, keepdims=True) > 0

    lines = []
    for f in range(8):
        w = pos[:, W * (f // 2) : W * (f // 2 + 1)]
        s = turn(w, AT)
        a, b = (w, s) if f % 2 == 0 else (s, w)
        lines.append((pair(a[0:1], b[1:2]), a[2:3]))
    x0, x1 = (jnp.concatenate([line[i] for line in lines], axis=0) for i in range(2))

    d = dens[...].astype(f32)
    energy = jnp.sum(d * terms[...].astype(f32))
    dd = jnp.concatenate([d, d], axis=1)
    side, half = iota(dd.shape, 0), iota(dd.shape, 1) // AT
    diag = jnp.concatenate(
        [jnp.where(side == 2 * j + half, dd, 0.0).astype(bf16) for j in range(SLOTS // 2)], axis=1
    )
    route = chosen.astype(f32).astype(bf16)[:, : 2 * SLOTS]
    weights = dot(route, jnp.concatenate([diag, diag], axis=0)).astype(bf16)

    for copy in copies[-PARTS:]:
        copy.wait()
    g = [dot(weights, ints[:, c].reshape(SLOTS * AT, W)) for c in range(3)]
    h = [turn(v, AT) for v in g]
    v0 = pair(jnp.where(second, h[0], g[0]), jnp.where(second, g[1], h[1]))
    v1 = jnp.where(second, h[2], g[2])
    shares = [jnp.where(col == PLACE, place, window(v0, v1, Q * y, Q, 0)) for y in range(Y)]
    at = iota((8, W), 1)
    for y in range(Y):
        extra = jnp.where(at == SCALAR, energy, window(x0, x1, Q * y, Q, AT))
        for k in range(XC):
            out[k * Y + YS.index(y)] = pair(shares[y][8 * k : 8 * (k + 1)], extra)


def turn_kernel(got, out):
    s = jnp.concatenate(
        [
            (got[k * Y] + got[k * Y + 1]) + (got[k * Y + 2] + got[k * Y + 3])
            for k in range(XC)
        ],
        axis=0,
    )
    row, col = iota(s.shape, 0), iota(s.shape, 1)
    place = s[:, PLACE : PLACE + 1].astype(i32)
    z, place = place >> 10, (place & 1023).astype(f32)
    z = jnp.broadcast_to(z, s.shape)
    again = (z == pltpu.roll(z, 1, 0)) & ((row & 7) != 0)
    to = z * XC + (row >> 3) + jnp.where(again, Z * XC, 0)
    to = jnp.where(row == (col & 63), to.astype(f32), 0.0)
    to = jnp.sum(to, axis=0, keepdims=True).astype(i32)
    r, c = iota((Z * XC, W), 0), iota((Z * XC, W), 1)
    route = (r + jnp.where(c < 64, 0, Z * XC) == to).astype(f32).astype(bf16)
    low = jnp.where(col < Q, s, jnp.where(col == PLACE, place, 0.0))
    hi, lo = split(jnp.concatenate([low, turn(low, AT)], axis=0))
    v = dot(route, hi) + dot(route, lo)
    energy = jnp.sum(jnp.where((row & 7) == 0, s, 0.0), axis=0, keepdims=True)
    v = jnp.where(iota(v.shape, 1) == SCALAR, energy, v)
    out[...] = v.reshape(Z, XC, W)


def block_kernel(got, first, out):
    v = got[...].reshape(Z * XC, W)
    row, col = iota(v.shape, 0), iota(v.shape, 1)
    upper = (col >= AT) & (col < AT + Q)
    f = iota((PLANE * 8, W), 0).astype(f32) * Y
    picks = []
    for p in (PLACE, AT + PLACE):
        place = jnp.sum(jnp.where(row == col, v[:, p : p + 1], 0.0), axis=0, keepdims=True)
        picks.append((place == f).astype(f32).astype(bf16))
    pick = jnp.concatenate(picks, axis=1)
    data = jnp.concatenate([jnp.where(upper, d, 0.0) for d in (turn(v, AT), v)], axis=0)
    hi, lo = split(data)
    block = dot(pick, hi) + dot(pick, lo)
    virial = -jnp.sum(block * first[...].reshape(block.shape)) / 3.0
    energy = jnp.sum(jnp.where((row & 7) == 0, v, 0.0), axis=0, keepdims=True) / (Z * PLANE)
    at = iota(block.shape, 1)
    lower = turn(pltpu.roll(block, PLANE * 8 - 4, 0), -Q)
    block = jnp.where(at < AT, lower, block)
    block = jnp.where(at == SCALAR, energy, jnp.where(at == SCALAR - 1, virial, block))
    for k in range(PLANE):
        out[k] = block[8 * k : 8 * k + 4]


def scalar_kernel(got, scalars):
    total = jnp.sum(got[:, 0:1, :], axis=0)
    scalars[...] = jnp.broadcast_to(total[None], scalars.shape)


def force_kernel(got, scalars, forces, energy, virial):
    total = jnp.sum(scalars[...], axis=0)
    energy[0] = total[0, SCALAR]
    virial[0] = total[0, SCALAR - 1]
    mine = [sum(got[k * Y + YS.index(y)] for k in range(XC)) for y in range(Y)]
    mine = [jnp.concatenate([turn(m, -AT), turn(m, Q - AT)], axis=0) for m in mine]
    lane = iota((8, W), 1)
    m1, m2 = turn(mine[1], Q), turn(mine[2], 2 * Q)
    u = jnp.where(lane < Q, mine[0], jnp.where(lane < 2 * Q, m1, m2))
    w = jnp.where(lane < 3 * Q - W, m2, turn(mine[3], 3 * Q - W))
    su, sw = turn(u, AT), turn(w, AT)
    for k in range(4):
        a, b = slice(2 * k, 2 * k + 1), slice(2 * k + 1, 2 * k + 2)
        cols = slice(W * k, W * (k + 1))
        forces[0:1, cols] = pair(u[a], su[b])
        forces[1:2, cols] = pair(su[a], u[b])
        forces[2:3, cols] = pair(w[a], sw[b])


VM = pl.BlockSpec(memory_space=pltpu.VMEM)
HBM = pl.BlockSpec(memory_space=pltpu.HBM)
SM = pl.BlockSpec(memory_space=pltpu.SMEM)


def call(kernel, outs, n, scratch=(), where=VM, spaces=None):
    return pl.pallas_call(
        kernel,
        out_shape=outs,
        in_specs=[where] * n,
        out_specs=spaces or jax.tree.map(lambda _: VM, outs),
        scratch_shapes=scratch,
        cost_estimate=pl.CostEstimate(flops=20_000_000, bytes_accessed=1 << 18, transcendentals=0),
        compiler_params=pltpu.CompilerParams(vmem_limit_bytes=16 << 20),
    )


def arr(*shape):
    return jax.ShapeDtypeStruct(shape, f32)


def over_z(v):
    return lax.all_to_all(v, "z", 0, 0, axis_index_groups=[ZS], tiled=True)


def over_plane(v):
    order = [xc * Y + y for xc in XCS for y in YS]
    return lax.all_to_all(v, ("x", "c", "y"), 0, 0, axis_index_groups=[order], tiled=True)


def on_device(integrals, density, energy_terms, positions, dimer_owners, dimer_local):
    args = (
        jnp.transpose(integrals, (0, 2, 1, 3)),
        density,
        energy_terms,
        dimer_owners.T,
        dimer_local.T,
        positions,
    )
    scratch = [pltpu.VMEM(a.shape, a.dtype) for a in args] + [pltpu.SemaphoreType.DMA((5 + PARTS,))]
    args = (pltpu.with_memory_space_constraint(a, pltpu.HBM) for a in args)
    first = over_plane(call(send_kernel, arr(PLANE, 8, W), 6, scratch, HBM)(*args))
    v = over_z(call(turn_kernel, arr(Z, XC, W), 1)(first))
    v = call(block_kernel, arr(PLANE, 4, W), 2)(v, first)
    v = over_plane(v)
    scalars = over_z(call(scalar_kernel, arr(Z, 1, W), 1)(v))
    outs = (arr(3, 8 * AT), arr(1), arr(1))
    forces, energy, virial = call(force_kernel, outs, 2, spaces=(VM, SM, SM))(v, scalars)
    return forces, energy.reshape(()), virial.reshape(())


def solution(mesh):
    split_mesh = Mesh(mesh.devices.reshape(X, Z, C, Y), ALL)
    placed = (
        P(DIMER, "y", None, None),
        P(DIMER, "y"),
        P(DIMER, "y"),
        P(None, ALL),
        P(DIMER, None),
        P(DIMER, None),
    )
    return jax.shard_map(
        on_device,
        mesh=split_mesh,
        in_specs=placed,
        out_specs=(P(None, ALL), P(), P()),
        check_vma=False,
    )
```

```python
import jax
import jax.numpy as jnp
from jax import lax
from jax.experimental import pallas as pl
from jax.experimental.pallas import tpu as pltpu
from jax.sharding import Mesh
from jax.sharding import PartitionSpec as P

X, Z, C, Y = 4, 16, 2, 4
XC = X * C
PLANE = XC * Y
AT = 64
W = 128
SLOTS = 32
Q = 48
PARTS = 4
PLACE, SCALAR = Q, 127
X0, C0, Y0, Z0, Z2 = 2, 1, 2, 10, 9
ZS = [(Z0 + k) % Z for k in range(Z)]
Z2S = [(Z2 + k) % Z for k in range(Z)]
YS = [(Y0 + k) % Y for k in range(Y)]
XCS = [(X0 + i) % X * C + (C0 + j) % C for i in range(X) for j in range(C)]
DIMER = ("x", "z", "c")
ALL = ("x", "z", "c", "y")
f32, bf16, i32 = jnp.float32, jnp.bfloat16, jnp.int32


def iota(shape, dim):
    return lax.broadcasted_iota(i32, shape, dim)


def split(v):
    hi = v.astype(bf16)
    return hi, (v - hi.astype(f32)).astype(bf16)


def dot(a, b, dims=((1,), (0,))):
    return lax.dot_general(a, b, (dims, ((), ())), preferred_element_type=f32)


def turn(v, by):
    by %= W
    return pltpu.roll(v, by, 1) if by else v


def pair(a, b):
    return jnp.where(iota(a.shape, 1) < AT, a, b)


def window(v0, v1, first, count, to):
    lane = iota(v0.shape, 1)
    inside = (lane >= to) & (lane < to + count)
    if first + count <= W:
        v = turn(v0, to - first)
    elif first >= W:
        v = turn(v1, to - first)
    else:
        v = jnp.where(lane < to + W - first, turn(v0, to - first), turn(v1, to - first))
    return jnp.where(inside, v, 0.0)


def send_kernel(h_ints, h_dens, h_terms, h_own, h_loc, h_pos, out, *scratch):
    ints, dens, terms, own, loc, pos, sems = scratch
    part = SLOTS // PARTS
    pairs = [(h_dens, dens), (h_own, own), (h_loc, loc), (h_pos, pos), (h_terms, terms)]
    pairs += [(h_ints.at[pl.ds(part * i, part)], ints.at[pl.ds(part * i, part)]) for i in range(PARTS)]
    copies = [pltpu.make_async_copy(a, b, sems.at[i]) for i, (a, b) in enumerate(pairs)]
    for copy in copies:
        copy.start()
    for copy in copies[:-PARTS]:
        copy.wait()

    o = jnp.concatenate([own[0:1], own[1:2]] * 2, axis=1)
    f = jnp.concatenate([loc[0:1], loc[1:2]] * 2, axis=1)
    z = ((o >> 1) - Z0) & (Z - 1)
    xc = (((o >> 5) - X0) & (X - 1)) * C + ((o & 1) ^ C0)
    f = ((((f >> 3) - Y0) & (Y - 1)) << 3) + (f & 7)
    row, col = iota((2 * SLOTS, W), 0), iota((2 * SLOTS, W), 1)
    key = ((z * 8 + xc) * SLOTS + f) * (2 * SLOTS) + (col[:1] & (2 * SLOTS - 1))
    key_of = jnp.sum(jnp.where(row == col, key.astype(f32), 0.0), axis=1, keepdims=True)
    turn_of = jnp.sum((key_of < key.astype(f32)).astype(f32), axis=0, keepdims=True).astype(i32)
    chosen = (row == (turn_of & 7) * 8 + (turn_of >> 3)) & (col < 2 * SLOTS)
    place = jnp.sum(jnp.where(chosen, (key >> 6).astype(f32), 0.0), axis=1, keepdims=True)
    second = jnp.sum(jnp.where(chosen & (col >= SLOTS), 1.0, 0.0), axis=1, keepdims=True) > 0

    lines = []
    for f in range(8):
        w = pos[:, W * (f // 2) : W * (f // 2 + 1)]
        s = turn(w, AT)
        a, b = (w, s) if f % 2 == 0 else (s, w)
        lines.append((pair(a[0:1], b[1:2]), a[2:3]))
    x0, x1 = (jnp.concatenate([line[i] for line in lines], axis=0) for i in range(2))

    d = dens[...].astype(f32)
    energy = jnp.sum(d * terms[...].astype(f32))
    dd = jnp.concatenate([d, d], axis=1)
    side, half = iota(dd.shape, 0), iota(dd.shape, 1) // AT
    diag = jnp.concatenate(
        [jnp.where(side == 2 * j + half, dd, 0.0).astype(bf16) for j in range(SLOTS // 2)], axis=1
    )
    route = chosen.astype(f32).astype(bf16)[:, : 2 * SLOTS]
    weights = dot(route, jnp.concatenate([diag, diag], axis=0)).astype(bf16)

    for copy in copies[-PARTS:]:
        copy.wait()
    g = [dot(weights, ints[:, c].reshape(SLOTS * AT, W)) for c in range(3)]
    h = [turn(v, AT) for v in g]
    v0 = pair(jnp.where(second, h[0], g[0]), jnp.where(second, g[1], h[1]))
    v1 = jnp.where(second, h[2], g[2])
    shares = [jnp.where(col == PLACE, place, window(v0, v1, Q * y, Q, 0)) for y in range(Y)]
    at = iota((8, W), 1)
    for y in range(Y):
        extra = jnp.where(at == SCALAR, energy, window(x0, x1, Q * y, Q, AT))
        for k in range(XC):
            out[k * Y + YS.index(y)] = pair(shares[y][8 * k : 8 * (k + 1)], extra)


def turn_kernel(got, out):
    s = jnp.concatenate(
        [
            (got[k * Y] + got[k * Y + 1]) + (got[k * Y + 2] + got[k * Y + 3])
            for k in range(XC)
        ],
        axis=0,
    )
    row, col = iota(s.shape, 0), iota(s.shape, 1)
    place = s[:, PLACE : PLACE + 1].astype(i32)
    z, place = place >> 10, (place & 1023).astype(f32)
    z = jnp.broadcast_to(z, s.shape)
    again = (z == pltpu.roll(z, 1, 0)) & ((row & 7) != 0)
    to = z * XC + (row >> 3) + jnp.where(again, Z * XC, 0)
    to = jnp.where(row == (col & 63), to.astype(f32), 0.0)
    to = jnp.sum(to, axis=0, keepdims=True).astype(i32)
    r, c = iota((Z * XC, W), 0), iota((Z * XC, W), 1)
    route = (r + jnp.where(c < 64, 0, Z * XC) == to).astype(f32).astype(bf16)
    low = jnp.where(col < Q, s, jnp.where(col == PLACE, place, 0.0))
    hi, lo = split(jnp.concatenate([low, turn(low, AT)], axis=0))
    v = dot(route, hi) + dot(route, lo)
    energy = jnp.sum(jnp.where((row & 7) == 0, s, 0.0), axis=0, keepdims=True)
    v = jnp.where(iota(v.shape, 1) == SCALAR, energy, v)
    out[...] = v.reshape(Z, XC, W)


def block_kernel(got, first, out):
    v = got[...].reshape(Z * XC, W)
    row, col = iota(v.shape, 0), iota(v.shape, 1)
    upper = (col >= AT) & (col < AT + Q)
    f = iota((PLANE * 8, W), 0).astype(f32) * Y
    picks = []
    for p in (PLACE, AT + PLACE):
        place = jnp.sum(jnp.where(row == col, v[:, p : p + 1], 0.0), axis=0, keepdims=True)
        picks.append((place == f).astype(f32).astype(bf16))
    pick = jnp.concatenate(picks, axis=1)
    data = jnp.concatenate([jnp.where(upper, d, 0.0) for d in (turn(v, AT), v)], axis=0)
    hi, lo = split(data)
    block = dot(pick, hi) + dot(pick, lo)
    virial = -jnp.sum(block * first[...].reshape(block.shape)) / 3.0
    energy = jnp.sum(jnp.where((row & 7) == 0, v, 0.0), axis=0, keepdims=True) / (Z * PLANE)
    at = iota(block.shape, 1)
    lower = turn(pltpu.roll(block, PLANE * 8 - 4, 0), -Q)
    block = jnp.where(at < AT, lower, block)
    block = jnp.where(at == SCALAR, energy, jnp.where(at == SCALAR - 1, virial, block))
    for k in range(PLANE):
        out[k] = block[8 * k : 8 * k + 4]


def scalar_kernel(got, scalars):
    total = jnp.sum(got[:, 0:1, :], axis=0)
    scalars[...] = jnp.broadcast_to(total[None], scalars.shape)


def force_kernel(got, scalars, forces, energy, virial):
    total = jnp.sum(scalars[...], axis=0)
    energy[0] = total[0, SCALAR]
    virial[0] = total[0, SCALAR - 1]
    mine = [sum(got[k * Y + YS.index(y)] for k in range(XC)) for y in range(Y)]
    mine = [jnp.concatenate([turn(m, -AT), turn(m, Q - AT)], axis=0) for m in mine]
    lane = iota((8, W), 1)
    m1, m2 = turn(mine[1], Q), turn(mine[2], 2 * Q)
    u = jnp.where(lane < Q, mine[0], jnp.where(lane < 2 * Q, m1, m2))
    w = jnp.where(lane < 3 * Q - W, m2, turn(mine[3], 3 * Q - W))
    su, sw = turn(u, AT), turn(w, AT)
    for k in range(4):
        a, b = slice(2 * k, 2 * k + 1), slice(2 * k + 1, 2 * k + 2)
        cols = slice(W * k, W * (k + 1))
        forces[0:1, cols] = pair(u[a], su[b])
        forces[1:2, cols] = pair(su[a], u[b])
        forces[2:3, cols] = pair(w[a], sw[b])


VM = pl.BlockSpec(memory_space=pltpu.VMEM)
HBM = pl.BlockSpec(memory_space=pltpu.HBM)
SM = pl.BlockSpec(memory_space=pltpu.SMEM)


def call(kernel, outs, n, scratch=(), where=VM, spaces=None):
    return pl.pallas_call(
        kernel,
        out_shape=outs,
        in_specs=[where] * n,
        out_specs=spaces or jax.tree.map(lambda _: VM, outs),
        scratch_shapes=scratch,
        cost_estimate=pl.CostEstimate(flops=20_000_000, bytes_accessed=1 << 18, transcendentals=0),
        compiler_params=pltpu.CompilerParams(vmem_limit_bytes=16 << 20),
    )


def arr(*shape):
    return jax.ShapeDtypeStruct(shape, f32)


def over_z(v, order):
    return lax.all_to_all(v, "z", 0, 0, axis_index_groups=[order], tiled=True)


def over_plane(v):
    order = [xc * Y + y for xc in XCS for y in YS]
    return lax.all_to_all(v, ("x", "c", "y"), 0, 0, axis_index_groups=[order], tiled=True)


def on_device(integrals, density, energy_terms, positions, dimer_owners, dimer_local):
    args = (
        jnp.transpose(integrals, (0, 2, 1, 3)),
        density,
        energy_terms,
        dimer_owners.T,
        dimer_local.T,
        positions,
    )
    scratch = [pltpu.VMEM(a.shape, a.dtype) for a in args] + [pltpu.SemaphoreType.DMA((5 + PARTS,))]
    args = (pltpu.with_memory_space_constraint(a, pltpu.HBM) for a in args)
    first = over_plane(call(send_kernel, arr(PLANE, 8, W), 6, scratch, HBM)(*args))
    v = over_z(call(turn_kernel, arr(Z, XC, W), 1)(first), ZS)
    v = call(block_kernel, arr(PLANE, 4, W), 2)(v, first)
    v = over_plane(v)
    scalars = over_z(call(scalar_kernel, arr(Z, 1, W), 1)(v), Z2S)
    outs = (arr(3, 8 * AT), arr(1), arr(1))
    forces, energy, virial = call(force_kernel, outs, 2, spaces=(VM, SM, SM))(v, scalars)
    return forces, energy.reshape(()), virial.reshape(())


def solution(mesh):
    split_mesh = Mesh(mesh.devices.reshape(X, Z, C, Y), ALL)
    placed = (
        P(DIMER, "y", None, None),
        P(DIMER, "y"),
        P(DIMER, "y"),
        P(None, ALL),
        P(DIMER, None),
        P(DIMER, None),
    )
    return jax.shard_map(
        on_device,
        mesh=split_mesh,
        in_specs=placed,
        out_specs=(P(None, ALL), P(), P()),
        check_vma=False,
    )
```
